128 devices in a mesh: grp: 64 (over z, y, x), loc: 2 (over core).
Axes of the slice: x: 4, y: 4, z: 4, core: 2. Of those that a mesh axis runs over, the one named last changes fastest.
Arguments:
- tokens: bfloat16 [4096, 3584], P(('grp', 'loc')), may hold values from -6 to 6
- gate_weights: bfloat16 [4096, 8], P(('grp', 'loc')), may hold values from 0.099609375 to 0.59765625
- expert_ids: int32 [4096, 8], P(('grp', 'loc')), may hold values from 0 to 127, as said below
- w_gate: bfloat16 [128, 3584, 1024], P('grp', None, 'loc'), may hold values from -0.09375 to 0.09375
- w_up: bfloat16 [128, 3584, 1024], P('grp', None, 'loc'), may hold values from -0.09375 to 0.09375
- w_down: bfloat16 [128, 3584, 1024], P('grp', None, 'loc'), may hold values from -0.1875 to 0.1875
Outputs:
- layer_out: bfloat16 [4096, 3584], P(('grp', 'loc'))
The draws below stay inside these ranges and needn't reach their ends.
Inputs may be any that keep to these rules, and one draw needn't show every extreme that they name: `expert_ids`: each row names 8 different experts: two in each of 4 different routing groups, a routing group being 16 consecutive expert numbers. Among the rows of one device (aligned blocks of 32 rows) each expert is named at most 4 times, and in every such block some expert is named exactly 4 times.
All inputs are finite; a program needn't handle non-finite values.
Results may differ from the reference program's by a relative error of at most 0.01.
Values may be sent and summed in bfloat16 or wider, within the bound.
A program may use at most 192 MiB of HBM per device.

```python
import jax
import jax.numpy as jnp
from jax import lax

D = 3584
FFE = 1024
RGROUPS = 8
TOPG = 4
TOPK = 8
TOK_DEV = 32
EXPERTS = 128
TOKENS = 4096
MOST = 4
N_LOC = 2


def draw_expert_ids(key, part):
    group_span = EXPERTS // RGROUPS
    block_count = TOKENS // TOK_DEV
    key_first = jax.random.fold_in(key, 11)
    key_second = jax.random.fold_in(key, 12)
    key_rank = jax.random.fold_in(key, 13)
    key_rotation = jax.random.fold_in(key, 14)
    hot_first = jax.random.randint(key_first, (block_count,), 0, RGROUPS)
    hot_second = jax.random.randint(key_second, (block_count,), 0, RGROUPS)
    hot_group = jnp.repeat(jnp.minimum(hot_first, hot_second), TOK_DEV)
    group_index = jnp.arange(RGROUPS, dtype=jnp.int32)
    scores = jax.random.randint(key_rank, (TOKENS, RGROUPS), 0, 1 << 20) * RGROUPS + group_index[None, :]
    scores = jnp.where(group_index[None, :] == hot_group[:, None], 1 << 30, scores)
    chosen = lax.top_k(scores, TOPG)[1].astype(jnp.int32)
    member = jnp.sum((chosen[:, :, None] == group_index[None, None, :]).astype(jnp.int32), axis=1)
    member = member.reshape(block_count, TOK_DEV, RGROUPS)
    order_rank = jnp.cumsum(member, axis=1) - member
    rotation = jax.random.randint(key_rotation, (block_count, 1, RGROUPS), 0, group_span)
    first_local = ((rotation + order_rank) % group_span).reshape(TOKENS, RGROUPS)
    first_pick = jnp.take_along_axis(first_local, chosen, axis=1)
    second_pick = (first_pick + group_span // 2) % group_span
    group_base = chosen * group_span
    expert_pick = jnp.stack([group_base + first_pick, group_base + second_pick], axis=2)
    return expert_pick.reshape(TOKENS, TOPK).astype(jnp.int32)


def shard_levels(rng, extent, pieces, least, high):
    def one(position, parts):
        heights = jax.random.uniform(jax.random.fold_in(jax.random.fold_in(rng, 6), position), (parts,), jnp.float32, least / len(pieces), high / len(pieces))
        return jnp.repeat(jnp.exp(heights), extent[position] // parts).reshape((-1,) + (1,) * (len(extent) - position - 1))

    level = one(*pieces[0])
    for cut in pieces[1:]:
        level = level * one(*cut)
    return level


def centred(own_key, extent, scale, limit, shards=(), kind=jnp.bfloat16):
    values = jax.random.normal(own_key, extent, jnp.float32) * scale
    if len(shards) > 0:
        values = shard_levels(own_key, extent, shards, -0.22, 0.18) * values
    return jnp.clip(values, min=-limit, max=limit).astype(kind)


def setup_inputs(seed: int = 0) -> dict:
    streams_of = jax.random.split(jax.random.key(seed), 7)
    tokens = centred(streams_of[0], (TOKENS, D), 1.0, 6.0, ((0, 128),))
    gate_weights = jnp.clip(0.099609375 + 0.49804688 * jax.random.uniform(streams_of[1], (TOKENS, TOPK), jnp.float32) ** shard_levels(streams_of[1], (TOKENS, TOPK), ((0, 128),), -0.2, 0.2), 0.099609375, 0.59765625).astype(jnp.bfloat16)
    expert_ids = draw_expert_ids(jax.random.fold_in(streams_of[6], 71), 0)
    w_gate = centred(streams_of[3], (EXPERTS, D, FFE), D ** -0.5, 0.09375, ((0, 64), (2, 2)))
    w_up = centred(streams_of[4], (EXPERTS, D, FFE), D ** -0.5, 0.09375, ((0, 64), (2, 2)))
    w_down = centred(streams_of[5], (EXPERTS, D, FFE), FFE ** -0.5, 0.1875, ((0, 64), (2, 2)))
    return dict(tokens=tokens, gate_weights=gate_weights, expert_ids=expert_ids, w_gate=w_gate, w_up=w_up, w_down=w_down)


def reference(tokens, gate_weights, expert_ids, w_gate, w_up, w_down):
    block_count = TOKENS // TOK_DEV
    pair_block = TOK_DEV * TOPK
    per_expert = block_count * MOST
    shard_units = FFE // N_LOC
    block_ids = expert_ids.reshape(block_count, pair_block).astype(jnp.int32)
    same_expert = (block_ids[:, :, None] == block_ids[:, None, :]).astype(jnp.int32)
    pair_order = jnp.arange(pair_block, dtype=jnp.int32)
    earlier = (pair_order[:, None] > pair_order[None, :]).astype(jnp.int32)
    slot_rank = jnp.sum(same_expert * earlier[None], axis=2).astype(jnp.int32)
    block_index = jnp.arange(block_count, dtype=jnp.int32)[:, None]
    target = (block_ids * per_expert + block_index * MOST + slot_rank).reshape(-1).astype(jnp.int32)
    pair_index = jnp.arange(TOKENS * TOPK, dtype=jnp.int32)
    slot_table = jnp.full((EXPERTS * per_expert,), -1, jnp.int32).at[target].set(pair_index)
    slot_table = slot_table.reshape(EXPERTS, per_expert)
    flat_scales = gate_weights.reshape(-1)

    def one_expert(totals, inputs):
        index_row, gate_part, up_part, down_part = inputs
        is_valid = index_row >= 0
        safe_index = jnp.maximum(index_row, 0).astype(jnp.int32)
        token_row = (safe_index // TOPK).astype(jnp.int32)
        rows_in = tokens[token_row]
        scales = jnp.where(is_valid, flat_scales[safe_index].astype(jnp.float32), jnp.zeros((), jnp.float32))
        gate_act = jnp.dot(rows_in, gate_part, preferred_element_type=jnp.float32)
        upward = jnp.dot(rows_in, up_part, preferred_element_type=jnp.float32)
        hidden = (jax.nn.silu(gate_act) * upward).astype(jnp.bfloat16)
        blocked = hidden.reshape(per_expert, N_LOC, shard_units).astype(jnp.float32)
        down_blocks = down_part.reshape(D, N_LOC, shard_units).astype(jnp.float32)
        partial_value = jnp.einsum("rlf,dlf->rld", blocked, down_blocks)
        partial_value = lax.optimization_barrier((partial_value * scales[:, None, None]).astype(jnp.bfloat16))
        outcome = jnp.sum(partial_value.astype(jnp.float32), axis=1).astype(jnp.bfloat16)
        outcome = lax.optimization_barrier(outcome)
        return totals.at[token_row].add(outcome.astype(jnp.float32)), None

    start_totals = jnp.zeros((TOKENS, D), jnp.float32)
    totals = lax.scan(one_expert, start_totals, (slot_table, w_gate, w_up, w_down))[0]
    return totals.astype(jnp.bfloat16)
```

```python
import jax
import jax.numpy as jnp
from jax import lax
from jax.experimental import pallas as pl
from jax.experimental.pallas import tpu as pltpu
from jax.sharding import PartitionSpec as P

SIDE = 4
CUBE = 8
MOST = 4
STEP = 512
LAG_IN = 2
LAG_BACK = 3
LAG_SUM = 5
F32 = jnp.float32
BF16 = jnp.bfloat16


def paired(coord, kind):
    odd = lax.rem(coord + kind, 2)
    return lax.rem(coord + SIDE + 1 - 2 * odd, SIDE)


def cube_of(place, kind):
    pairs = [(coord, paired(coord, kind)) for coord in place]
    return [
        (pairs[0][d // 4] * SIDE + pairs[1][d // 2 % 2]) * SIDE + pairs[2][d % 2]
        for d in range(CUBE)
    ]


def dot(left, right):
    return jnp.dot(left, right, preferred_element_type=F32)


def kernel(
    tokens, scales, ids, w_gate, w_up, w_down, out,
    held, table, pick, mix, sent, rows, gate_acc, up_acc, hidden, made, back, part, last,
    gate_v, up_v, down_v,
    tok_sem, table_sems, s1, s2, s3, s4, w_local, w_send, w_recv,
):
    count = tokens.shape[0]
    steps = held.shape[0]
    block = CUBE * MOST
    slots = 2 * CUBE * block
    me = lax.axis_index("grp")
    core = lax.axis_index("loc")
    other = 1 - core
    place = (me // (SIDE * SIDE), lax.rem(me // SIDE, SIDE), lax.rem(me, SIDE))
    near = cube_of(place, core)
    far = cube_of(place, other)

    def feature_span(step):
        return pl.ds(pl.multiple_of(step * STEP, STEP), STEP)

    def token_load(step):
        return pltpu.make_async_copy(
            tokens.at[:, feature_span(step)], held.at[step, pl.ds(0, count)], tok_sem.at[step]
        )

    def weight_load(which, step):
        source = (w_gate, w_up, w_down)[which]
        target = (gate_v, up_v, down_v)[which]
        return pltpu.make_async_copy(
            source.at[core, feature_span(step)], target.at[step, 0], w_local.at[which, step]
        )

    def weight_send(which, step):
        source = (w_gate, w_up, w_down)[which]
        target = (gate_v, up_v, down_v)[which]
        return pltpu.make_async_remote_copy(
            src_ref=source.at[other, feature_span(step)],
            dst_ref=target.at[step, 1],
            send_sem=w_send.at[which, step],
            recv_sem=w_recv.at[which, step],
            device_id={"grp": me, "loc": other},
            device_id_type=pl.DeviceIdType.MESH,
        )

    def send(source, target, sems, chip, to_core):
        pltpu.make_async_remote_copy(
            src_ref=source,
            dst_ref=target,
            send_sem=sems[0],
            recv_sem=sems[1],
            device_id={"grp": chip, "loc": to_core},
            device_id_type=pl.DeviceIdType.MESH,
        ).start()

    def wait_for(ref, sem):
        pltpu.make_async_copy(ref, ref, sem).wait()

    for step in range(steps):
        token_load(step).start()
    barrier = pltpu.get_barrier_semaphore()
    partners = [(me, other)]
    for d in range(1, CUBE):
        partners += [(near[d], core), (near[d], other), (far[d], core), (far[d], other)]
    for chip, to_core in partners:
        pl.semaphore_signal(
            barrier, inc=1, device_id={"grp": chip, "loc": to_core},
            device_id_type=pl.DeviceIdType.MESH,
        )

    def start_weights(step, carry):
        for which in range(3):
            weight_load(which, step).start()
        return carry

    lax.fori_loop(0, steps, start_weights, 0)

    expert_line = lax.broadcasted_iota(jnp.int32, (count, 128), 1)
    chosen = jnp.zeros((count, 128), F32)
    weight_of = jnp.zeros((count, 128), F32)
    for k in range(ids.shape[1]):
        match = ids[:, k : k + 1] == expert_line
        chosen = chosen + jnp.where(match, 1.0, 0.0)
        weight_of = weight_of + jnp.where(match, scales[:, k : k + 1].astype(F32), 0.0)
    before = (
        lax.broadcasted_iota(jnp.int32, (count, count), 1)
        < lax.broadcasted_iota(jnp.int32, (count, count), 0)
    )
    earlier = dot(jnp.where(before, 1.0, 0.0).astype(BF16), chosen.astype(BF16))
    table[0, :count] = (chosen * (earlier + 1.0)).astype(BF16)
    table[0, count:] = weight_of.astype(BF16)
    gate_acc[...] = jnp.zeros_like(gate_acc)
    up_acc[...] = jnp.zeros_like(up_acc)

    pl.semaphore_wait(barrier, len(partners))

    for d in range(1, CUBE):
        send(table.at[0], table.at[d], (table_sems.at[0], table_sems.at[1]), near[d], core)

    def spread(step, carry):
        token_load(step).wait()
        for d in range(1, CUBE):
            send(
                held.at[step, pl.ds(0, count)], held.at[step, pl.ds(d * count, count)],
                (s1.at[0, step], s1.at[1, step]), near[d], core,
            )
        return carry

    lax.fori_loop(0, steps, spread, 0)

    slot = lax.broadcasted_iota(jnp.int32, (1, slots), 1)
    slot_core = slot // (CUBE * block)
    slot_chip = slot // block % CUBE
    slot_source = slot // MOST % CUBE
    slot_rank = slot % MOST
    pairs = [(coord, paired(coord, other)) for coord in place]
    chip = (
        jnp.where(slot_chip // 4 == 0, pairs[0][0], pairs[0][1]) * SIDE
        + jnp.where(slot_chip // 2 % 2 == 0, pairs[1][0], pairs[1][1])
    ) * SIDE + jnp.where(slot_chip % 2 == 0, pairs[2][0], pairs[2][1])
    slot_expert = chip * 2 + (core + slot_core) % 2
    widen = jnp.where(
        lax.broadcasted_iota(jnp.int32, (128, slots), 0) == slot_expert, 1.0, 0.0
    ).astype(BF16)

    wait_for(table.at[pl.ds(1, CUBE - 1)], table_sems.at[1])
    codes = jnp.concatenate([table[d, :count] for d in range(CUBE)], axis=0)
    weights = jnp.concatenate([table[d, count:] for d in range(CUBE)], axis=0)
    token_source = lax.broadcasted_iota(jnp.int32, (CUBE * count, 1), 0) // count
    hit = (dot(codes, widen) == (slot_rank + 1).astype(F32)) & (token_source == slot_source)
    mix[...] = jnp.where(hit, dot(weights, widen), 0.0).astype(BF16)
    pick[...] = jnp.where(hit, 1.0, 0.0).T.astype(BF16)

    def select(step):
        wait_for(held.at[step, pl.ds(count, (CUBE - 1) * count)], s1.at[1, step])
        chosen_rows = dot(pick[...], held[step]).astype(BF16)
        sent[step] = chosen_rows
        rows[step, :block] = chosen_rows[:block]
        for across in range(2):
            for d in range(CUBE):
                if across + d > 0:
                    span = pl.ds((across * CUBE + d) * block, block)
                    send(
                        sent.at[step, span], rows.at[step, span], (s2.at[0, step], s2.at[1, step]),
                        far[d], other if across else core,
                    )
        for which in range(3):
            weight_send(which, step).start()

    def accumulate(step):
        for which in range(2):
            weight_load(which, step).wait()
            weight_send(which, step).wait_recv()
        wait_for(rows.at[step, pl.ds(block, slots - block)], s2.at[1, step])
        arrived = rows[step]
        half = gate_v.shape[3]
        for h in range(2):
            gate_acc[:, h * half : (h + 1) * half] += dot(arrived, gate_v[step, h])
            up_acc[:, h * half : (h + 1) * half] += dot(arrived, up_v[step, h])

    def inward(turn, carry):
        @pl.when(turn < steps)
        def _():
            select(turn)

        @pl.when(turn >= LAG_IN)
        def _():
            accumulate(turn - LAG_IN)

        return carry

    lax.fori_loop(0, steps + LAG_IN, inward, 0)

    gate = gate_acc[...]
    hidden[...] = (gate / (1.0 + jnp.exp(-gate)) * up_acc[...]).astype(BF16)

    def project(step):
        weight_load(2, step).wait()
        weight_send(2, step).wait_recv()
        half = down_v.shape[3]
        total = None
        for h in range(2):
            term = lax.dot_general(
                hidden[:, h * half : (h + 1) * half], down_v[step, h], (((1,), (1,)), ((), ())),
                preferred_element_type=F32,
            )
            total = term if total is None else total + term
        result = total.astype(BF16)
        made[step] = result
        back[step, :block] = result[:block]
        for across in range(2):
            for d in range(CUBE):
                if across + d > 0:
                    span = pl.ds((across * CUBE + d) * block, block)
                    send(
                        made.at[step, span], back.at[step, span], (s3.at[0, step], s3.at[1, step]),
                        near[d] if across else far[d], other if across else core,
                    )

    def combine(step):
        wait_for(back.at[step, pl.ds(block, slots - block)], s3.at[1, step])
        sums = dot(mix[...], back[step]).astype(BF16)
        part[step] = sums
        last[step, :count] = sums[:count]
        for d in range(1, CUBE):
            span = pl.ds(d * count, count)
            send(
                part.at[step, span], last.at[step, span], (s4.at[0, step], s4.at[1, step]),
                near[d], core,
            )

    def finish(step):
        wait_for(last.at[step, pl.ds(count, (CUBE - 1) * count)], s4.at[1, step])
        total = last[step, :count].astype(F32)
        for d in range(1, CUBE):
            total = total + last[step, d * count : (d + 1) * count].astype(F32)
        out[:, feature_span(step)] = total.astype(BF16)

    def outward(turn, carry):
        @pl.when(turn < steps)
        def _():
            project(turn)

        @pl.when((turn >= LAG_BACK) & (turn < steps + LAG_BACK))
        def _():
            combine(turn - LAG_BACK)

        @pl.when(turn >= LAG_SUM)
        def _():
            finish(turn - LAG_SUM)

        return carry

    lax.fori_loop(0, steps + LAG_SUM, outward, 0)

    wait_for(table.at[pl.ds(1, CUBE - 1)], table_sems.at[0])

    def drain(step, carry):
        wait_for(held.at[step, pl.ds(count, (CUBE - 1) * count)], s1.at[0, step])
        wait_for(sent.at[step, pl.ds(block, slots - block)], s2.at[0, step])
        wait_for(made.at[step, pl.ds(block, slots - block)], s3.at[0, step])
        wait_for(part.at[step, pl.ds(count, (CUBE - 1) * count)], s4.at[0, step])
        for which in range(3):
            weight_send(which, step).wait_send()
        return carry

    lax.fori_loop(0, steps, drain, 0)


def body(tokens, gate_weights, expert_ids, w_gate, w_up, w_down):
    count, features = tokens.shape
    units = w_gate.shape[2]
    steps = features // STEP
    gathered = CUBE * count
    slots = 2 * CUBE * CUBE * MOST
    dma = pltpu.SemaphoreType.DMA
    whole = pl.BlockSpec(memory_space=pl.ANY)
    vmem = pl.BlockSpec(memory_space=pltpu.VMEM)
    return pl.pallas_call(
        kernel,
        out_shape=jax.ShapeDtypeStruct((count, features), BF16),
        in_specs=[whole, vmem, vmem, whole, whole, whole],
        out_specs=vmem,
        scratch_shapes=[
            pltpu.VMEM((steps, gathered, STEP), BF16),
            pltpu.VMEM((CUBE, 2 * count, 128), BF16),
            pltpu.VMEM((slots, gathered), BF16),
            pltpu.VMEM((gathered, slots), BF16),
            pltpu.VMEM((steps, slots, STEP), BF16),
            pltpu.VMEM((steps, slots, STEP), BF16),
            pltpu.VMEM((slots, 2 * units), F32),
            pltpu.VMEM((slots, 2 * units), F32),
            pltpu.VMEM((slots, 2 * units), BF16),
            pltpu.VMEM((steps, slots, STEP), BF16),
            pltpu.VMEM((steps, slots, STEP), BF16),
            pltpu.VMEM((steps, gathered, STEP), BF16),
            pltpu.VMEM((steps, gathered, STEP), BF16),
            pltpu.VMEM((steps, 2, STEP, units), BF16),
            pltpu.VMEM((steps, 2, STEP, units), BF16),
            pltpu.VMEM((steps, 2, STEP, units), BF16),
            dma((steps,)),
            dma((2,)),
            dma((2, steps)),
            dma((2, steps)),
            dma((2, steps)),
            dma((2, steps)),
            dma((3, steps)),
            dma((3, steps)),
            dma((3, steps)),
        ],
        compiler_params=pltpu.CompilerParams(
            collective_id=0, has_side_effects=True, vmem_limit_bytes=66_000_000
        ),
    )(tokens, gate_weights, expert_ids, w_gate, w_up, w_down)


def solution(mesh):
    placed = (
        P(("grp", "loc"), None),
        P(("grp", "loc"), None),
        P(("grp", "loc"), None),
        P("grp", None, "loc"),
        P("grp", None, "loc"),
        P("grp", None, "loc"),
    )
    return jax.shard_map(
        body, mesh=mesh, in_specs=placed, out_specs=P(("grp", "loc"), None), check_vma=False
    )
```

```python
import jax
import jax.numpy as jnp
from jax import lax
from jax.experimental import pallas as pl
from jax.experimental.pallas import tpu as pltpu
from jax.sharding import PartitionSpec as P

SIDE = 4
CUBE = 8
MOST = 4
STEP = 512
LAG_SUM = 3
F32 = jnp.float32
BF16 = jnp.bfloat16


def paired(coord, kind):
    odd = lax.rem(coord + kind, 2)
    return lax.rem(coord + SIDE + 1 - 2 * odd, SIDE)


def cube_of(place, kind):
    pairs = [(coord, paired(coord, kind)) for coord in place]
    return [
        (pairs[0][d // 4] * SIDE + pairs[1][d // 2 % 2]) * SIDE + pairs[2][d % 2]
        for d in range(CUBE)
    ]


def dot(left, right):
    return jnp.dot(left, right, preferred_element_type=F32)


def dot_t(left, right):
    return lax.dot_general(left, right, (((1,), (1,)), ((), ())), preferred_element_type=F32)


def kernel(
    tokens, scales, ids, w_gate, w_up, w_down, out,
    held, table, pick, mix, sent, rows, gate_acc, up_acc, hidden, made, back, part, last,
    gate_v, up_v, down_v,
    tok_sem, table_sems, s1, s2, s3, s4, w_local, w_send, w_recv,
):
    count = tokens.shape[0]
    steps = held.shape[0]
    block = CUBE * MOST
    slots = 2 * CUBE * block
    me = lax.axis_index("grp")
    core = lax.axis_index("loc")
    other = 1 - core
    place = (me // (SIDE * SIDE), lax.rem(me // SIDE, SIDE), lax.rem(me, SIDE))
    near = cube_of(place, core)
    far = cube_of(place, other)

    def feature_span(step):
        return pl.ds(pl.multiple_of(step * STEP, STEP), STEP)

    def token_load(step):
        return pltpu.make_async_copy(
            tokens.at[:, feature_span(step)], held.at[step, pl.ds(0, count)], tok_sem.at[step]
        )

    def weight_load(which, step):
        source = (w_gate, w_up, w_down)[which]
        target = (gate_v, up_v, down_v)[which]
        return pltpu.make_async_copy(
            source.at[core, feature_span(step)], target.at[step, 0], w_local.at[which, step]
        )

    def weight_send(which, step):
        source = (w_gate, w_up, w_down)[which]
        target = (gate_v, up_v, down_v)[which]
        return pltpu.make_async_remote_copy(
            src_ref=source.at[other, feature_span(step)],
            dst_ref=target.at[step, 1],
            send_sem=w_send.at[which, step],
            recv_sem=w_recv.at[which, step],
            device_id={"grp": me, "loc": other},
            device_id_type=pl.DeviceIdType.MESH,
        )

    def send(source, target, sems, chip, to_core):
        pltpu.make_async_remote_copy(
            src_ref=source,
            dst_ref=target,
            send_sem=sems[0],
            recv_sem=sems[1],
            device_id={"grp": chip, "loc": to_core},
            device_id_type=pl.DeviceIdType.MESH,
        ).start()

    def wait_for(ref, sem):
        pltpu.make_async_copy(ref, ref, sem).wait()

    for step in range(steps):
        token_load(step).start()
    barrier = pltpu.get_barrier_semaphore()
    partners = [(me, other)]
    for d in range(1, CUBE):
        partners += [(near[d], core), (near[d], other), (far[d], core), (far[d], other)]
    for chip, to_core in partners:
        pl.semaphore_signal(
            barrier, inc=1, device_id={"grp": chip, "loc": to_core},
            device_id_type=pl.DeviceIdType.MESH,
        )

    def start_weights(step, carry):
        for which in range(3):
            weight_load(which, step).start()
        return carry

    lax.fori_loop(0, steps, start_weights, 0)

    expert_row = lax.broadcasted_iota(jnp.int32, (128, count), 0)
    chosen = jnp.zeros((128, count), F32)
    weight_of = jnp.zeros((128, count), F32)
    for k in range(ids.shape[0]):
        match = ids[k : k + 1, :] == expert_row
        chosen = chosen + jnp.where(match, 1.0, 0.0)
        weight_of = weight_of + jnp.where(match, scales[k : k + 1, :].astype(F32), 0.0)
    column = lax.broadcasted_iota(jnp.int32, (count, count), 1)
    row = lax.broadcasted_iota(jnp.int32, (count, count), 0)
    same = jnp.where(column == row, 1.0, 0.0).astype(BF16)
    before = jnp.where(column < row, 1.0, 0.0).astype(BF16)
    chosen = chosen.astype(BF16)
    table[0, :count] = (dot_t(same, chosen) * (dot_t(before, chosen) + 1.0)).astype(BF16)
    table[0, count:] = dot_t(same, weight_of.astype(BF16)).astype(BF16)
    gate_acc[...] = jnp.zeros_like(gate_acc)
    up_acc[...] = jnp.zeros_like(up_acc)

    pl.semaphore_wait(barrier, len(partners))

    for d in range(1, CUBE):
        send(table.at[0], table.at[d], (table_sems.at[0], table_sems.at[1]), near[d], core)

    def spread(step, carry):
        token_load(step).wait()
        for d in range(1, CUBE):
            send(
                held.at[step, pl.ds(0, count)], held.at[step, pl.ds(d * count, count)],
                (s1.at[0, step], s1.at[1, step]), near[d], core,
            )
        return carry

    lax.fori_loop(0, steps, spread, 0)

    slot = lax.broadcasted_iota(jnp.int32, (1, slots), 1)
    slot_core = slot // (CUBE * block)
    slot_chip = slot // block % CUBE
    slot_source = slot // MOST % CUBE
    slot_rank = slot % MOST
    pairs = [(coord, paired(coord, other)) for coord in place]
    chip = (
        jnp.where(slot_chip // 4 == 0, pairs[0][0], pairs[0][1]) * SIDE
        + jnp.where(slot_chip // 2 % 2 == 0, pairs[1][0], pairs[1][1])
    ) * SIDE + jnp.where(slot_chip % 2 == 0, pairs[2][0], pairs[2][1])
    slot_expert = chip * 2 + (core + slot_core) % 2
    widen = jnp.where(
        lax.broadcasted_iota(jnp.int32, (128, slots), 0) == slot_expert, 1.0, 0.0
    ).astype(BF16)

    wait_for(table.at[pl.ds(1, CUBE - 1)], table_sems.at[1])
    codes = jnp.concatenate([table[d, :count] for d in range(CUBE)], axis=0)
    weights = jnp.concatenate([table[d, count:] for d in range(CUBE)], axis=0)
    token_source = lax.broadcasted_iota(jnp.int32, (CUBE * count, 1), 0) // count
    hit = (dot(codes, widen) == (slot_rank + 1).astype(F32)) & (token_source == slot_source)
    mix[...] = jnp.where(hit, dot(weights, widen), 0.0).astype(BF16)
    pick[...] = jnp.where(hit, 1.0, 0.0).T.astype(BF16)

    def half_span(across):
        low = across * CUBE * block
        return pl.ds(low + block * (1 - across), CUBE * block - block * (1 - across))

    def send_rows(across, step):
        for d in range(across == 0, CUBE):
            span = pl.ds((across * CUBE + d) * block, block)
            send(
                sent.at[step, span], rows.at[step, span],
                (s2.at[0, across, step], s2.at[1, across, step]),
                far[d], other if across else core,
            )

    def select(step):
        wait_for(held.at[step, pl.ds(count, (CUBE - 1) * count)], s1.at[1, step])
        chosen_rows = dot(pick[...], held[step]).astype(BF16)
        sent[step] = chosen_rows
        rows[step, :block] = chosen_rows[:block]
        send_rows(0, step)
        for which in range(3):
            weight_send(which, step).start()

    def inward(step, carry):
        select(step)
        return carry

    lax.fori_loop(0, steps, inward, 0)

    def second_half(step, carry):
        send_rows(1, step)
        return carry

    lax.fori_loop(0, steps, second_half, 0)

    half = gate_v.shape[3]
    for across in range(2):
        low = across * CUBE * block
        these = slice(low, low + CUBE * block)

        def accumulate(step, carry):
            if across == 0:
                for which in range(2):
                    weight_load(which, step).wait()
                    weight_send(which, step).wait_recv()
            wait_for(rows.at[step, half_span(across)], s2.at[1, across, step])
            arrived = rows[step, these]
            for h in range(2):
                gate_acc[these, h * half : (h + 1) * half] += dot(arrived, gate_v[step, h])
                up_acc[these, h * half : (h + 1) * half] += dot(arrived, up_v[step, h])
            return carry

        lax.fori_loop(0, steps, accumulate, 0)
        gate = gate_acc[these]
        hidden[these] = (gate / (1.0 + jnp.exp(-gate)) * up_acc[these]).astype(BF16)

        def project(step, carry):
            if across == 0:
                weight_load(2, step).wait()
                weight_send(2, step).wait_recv()
            result = (
                dot_t(hidden[these, :half], down_v[step, 0])
                + dot_t(hidden[these, half:], down_v[step, 1])
            ).astype(BF16)
            made[step, these] = result
            if across == 0:
                back[step, :block] = result[:block]
            for d in range(across == 0, CUBE):
                span = pl.ds((across * CUBE + d) * block, block)
                send(
                    made.at[step, span], back.at[step, span],
                    (s3.at[0, across, step], s3.at[1, across, step]),
                    near[d] if across else far[d], other if across else core,
                )
            return carry

        lax.fori_loop(0, steps, project, 0)

    def combine(step):
        for across in range(2):
            wait_for(back.at[step, half_span(across)], s3.at[1, across, step])
        sums = dot(mix[...], back[step]).astype(BF16)
        part[step] = sums
        last[step, :count] = sums[:count]
        for d in range(1, CUBE):
            span = pl.ds(d * count, count)
            send(
                part.at[step, span], last.at[step, span], (s4.at[0, step], s4.at[1, step]),
                near[d], core,
            )

    def finish(step):
        wait_for(last.at[step, pl.ds(count, (CUBE - 1) * count)], s4.at[1, step])
        total = last[step, :count].astype(F32)
        for d in range(1, CUBE):
            total = total + last[step, d * count : (d + 1) * count].astype(F32)
        out[:, feature_span(step)] = total.astype(BF16)

    def outward(turn, carry):
        @pl.when(turn < steps)
        def _():
            combine(turn)

        @pl.when(turn >= LAG_SUM)
        def _():
            finish(turn - LAG_SUM)

        return carry

    lax.fori_loop(0, steps + LAG_SUM, outward, 0)

    wait_for(table.at[pl.ds(1, CUBE - 1)], table_sems.at[0])

    def drain(step, carry):
        wait_for(held.at[step, pl.ds(count, (CUBE - 1) * count)], s1.at[0, step])
        for across in range(2):
            wait_for(sent.at[step, half_span(across)], s2.at[0, across, step])
            wait_for(made.at[step, half_span(across)], s3.at[0, across, step])
        wait_for(part.at[step, pl.ds(count, (CUBE - 1) * count)], s4.at[0, step])
        for which in range(3):
            weight_send(which, step).wait_send()
        return carry

    lax.fori_loop(0, steps, drain, 0)


def body(tokens, gate_weights, expert_ids, w_gate, w_up, w_down):
    count, features = tokens.shape
    units = w_gate.shape[2]
    steps = features // STEP
    gathered = CUBE * count
    slots = 2 * CUBE * CUBE * MOST
    dma = pltpu.SemaphoreType.DMA
    whole = pl.BlockSpec(memory_space=pl.ANY)
    vmem = pl.BlockSpec(memory_space=pltpu.VMEM)
    return pl.pallas_call(
        kernel,
        out_shape=jax.ShapeDtypeStruct((count, features), BF16),
        in_specs=[whole, vmem, vmem, whole, whole, whole],
        out_specs=vmem,
        scratch_shapes=[
            pltpu.VMEM((steps, gathered, STEP), BF16),
            pltpu.VMEM((CUBE, 2 * count, 128), BF16),
            pltpu.VMEM((slots, gathered), BF16),
            pltpu.VMEM((gathered, slots), BF16),
            pltpu.VMEM((steps, slots, STEP), BF16),
            pltpu.VMEM((steps, slots, STEP), BF16),
            pltpu.VMEM((slots, 2 * units), F32),
            pltpu.VMEM((slots, 2 * units), F32),
            pltpu.VMEM((slots, 2 * units), BF16),
            pltpu.VMEM((steps, slots, STEP), BF16),
            pltpu.VMEM((steps, slots, STEP), BF16),
            pltpu.VMEM((steps, gathered, STEP), BF16),
            pltpu.VMEM((steps, gathered, STEP), BF16),
            pltpu.VMEM((steps, 2, STEP, units), BF16),
            pltpu.VMEM((steps, 2, STEP, units), BF16),
            pltpu.VMEM((steps, 2, STEP, units), BF16),
            dma((steps,)),
            dma((2,)),
            dma((2, steps)),
            dma((2, 2, steps)),
            dma((2, 2, steps)),
            dma((2, steps)),
            dma((3, steps)),
            dma((3, steps)),
            dma((3, steps)),
        ],
        compiler_params=pltpu.CompilerParams(
            collective_id=0, has_side_effects=True, vmem_limit_bytes=66_000_000
        ),
    )(tokens, gate_weights.T, expert_ids.T, w_gate, w_up, w_down)


def solution(mesh):
    placed = (
        P(("grp", "loc"), None),
        P(("grp", "loc"), None),
        P(("grp", "loc"), None),
        P("grp", None, "loc"),
        P("grp", None, "loc"),
        P("grp", None, "loc"),
    )
    return jax.shard_map(
        body, mesh=mesh, in_specs=placed, out_specs=P(("grp", "loc"), None), check_vma=False
    )
```

```python
import jax
import jax.numpy as jnp
from jax import lax
from jax.experimental import pallas as pl
from jax.experimental.pallas import tpu as pltpu
from jax.sharding import PartitionSpec as P

SIDE = 4
CUBE = 8
MOST = 4
STEP = 896
ORDER = (7, 3, 5, 6, 1, 2, 4)
ONE_AWAY = (1, 2, 4)
ON = (2, 4, 1)
F32 = jnp.float32
BF16 = jnp.bfloat16


def paired(coord, kind):
    odd = lax.rem(coord + kind, 2)
    return lax.rem(coord + SIDE + 1 - 2 * odd, SIDE)


def cube_of(place, kind):
    pairs = [(coord, paired(coord, kind)) for coord in place]
    return [
        (pairs[0][d // 4] * SIDE + pairs[1][d // 2 % 2]) * SIDE + pairs[2][d % 2]
        for d in range(CUBE)
    ]


def dot(left, right):
    return jnp.dot(left, right, preferred_element_type=F32)


def dot_t(left, right):
    return lax.dot_general(left, right, (((1,), (1,)), ((), ())), preferred_element_type=F32)


def kernel(
    tokens, scales, ids, w_gate, w_up, w_down, out,
    held, table, pick, mix, sent, rows, gate_acc, up_acc, hidden, made, back, part, last, moved,
    gate_v, up_v, down_v,
    tok_sem, table_sems, s1, s2, s3, s4, w_local, w_send, w_recv,
):
    count = tokens.shape[0]
    steps = held.shape[0]
    block = CUBE * MOST
    slots = 2 * CUBE * block
    me = lax.axis_index("grp")
    core = lax.axis_index("loc")
    other = 1 - core
    place = (me // (SIDE * SIDE), lax.rem(me // SIDE, SIDE), lax.rem(me, SIDE))
    near = cube_of(place, core)
    far = cube_of(place, other)

    def feature_span(step):
        return pl.ds(pl.multiple_of(step * STEP, STEP), STEP)

    def token_load(step):
        return pltpu.make_async_copy(
            tokens.at[:, feature_span(step)], held.at[step, pl.ds(0, count)], tok_sem.at[step]
        )

    def weight_load(which, step):
        source = (w_gate, w_up, w_down)[which]
        target = (gate_v, up_v, down_v)[which]
        return pltpu.make_async_copy(
            source.at[core, feature_span(step)], target.at[step, 0], w_local.at[which, step]
        )

    def weight_send(which, step):
        source = (w_gate, w_up, w_down)[which]
        target = (gate_v, up_v, down_v)[which]
        return pltpu.make_async_remote_copy(
            src_ref=source.at[other, feature_span(step)],
            dst_ref=target.at[step, 1],
            send_sem=w_send.at[which, step],
            recv_sem=w_recv.at[which, step],
            device_id={"grp": me, "loc": other},
            device_id_type=pl.DeviceIdType.MESH,
        )

    def send(source, target, sems, chip, to_core):
        pltpu.make_async_remote_copy(
            src_ref=source,
            dst_ref=target,
            send_sem=sems[0],
            recv_sem=sems[1],
            device_id={"grp": chip, "loc": to_core},
            device_id_type=pl.DeviceIdType.MESH,
        ).start()

    def wait_for(ref, sem):
        pltpu.make_async_copy(ref, ref, sem).wait()

    def pass_tokens(step, block_here, block_there, chip, phase):
        send(
            held.at[step, pl.ds(block_here * count, count)],
            held.at[step, pl.ds(block_there * count, count)],
            (s1.at[0, phase, step], s1.at[1, phase, step]), chip, core,
        )

    for step in range(steps):
        token_load(step).start()
    barrier = pltpu.get_barrier_semaphore()
    partners = [(me, other)]
    for d in range(1, CUBE):
        partners += [(near[d], core), (near[d], other), (far[d], core), (far[d], other)]
    for chip, to_core in partners:
        pl.semaphore_signal(
            barrier, inc=1, device_id={"grp": chip, "loc": to_core},
            device_id_type=pl.DeviceIdType.MESH,
        )

    def start_weights(step, carry):
        for which in range(3):
            weight_load(which, step).start()
        return carry

    lax.fori_loop(0, steps, start_weights, 0)

    expert_row = lax.broadcasted_iota(jnp.int32, (128, count), 0)
    chosen = jnp.zeros((128, count), F32)
    weight_of = jnp.zeros((128, count), F32)
    for k in range(ids.shape[0]):
        match = ids[k : k + 1, :] == expert_row
        chosen = chosen + jnp.where(match, 1.0, 0.0)
        weight_of = weight_of + jnp.where(match, scales[k : k + 1, :].astype(F32), 0.0)
    column = lax.broadcasted_iota(jnp.int32, (count, count), 1)
    row = lax.broadcasted_iota(jnp.int32, (count, count), 0)
    same = jnp.where(column == row, 1.0, 0.0).astype(BF16)
    before = jnp.where(column < row, 1.0, 0.0).astype(BF16)
    chosen = chosen.astype(BF16)
    table[0, :count] = (dot_t(same, chosen) * (dot_t(before, chosen) + 1.0)).astype(BF16)
    table[0, count:] = dot_t(same, weight_of.astype(BF16)).astype(BF16)
    gate_acc[...] = jnp.zeros_like(gate_acc)
    up_acc[...] = jnp.zeros_like(up_acc)

    pl.semaphore_wait(barrier, len(partners))

    for step in range(steps):
        token_load(step).wait()
        for d in ONE_AWAY:
            pass_tokens(step, 0, d, near[d], 0)
        if step == 0:
            for d in ORDER:
                send(table.at[0], table.at[d], (table_sems.at[0], table_sems.at[1]), near[d], core)

    for step in range(steps):
        wait_for(held.at[step, pl.ds(0, len(ONE_AWAY) * count)], s1.at[1, 0, step])
        via = step % len(ONE_AWAY)
        pass_tokens(step, ONE_AWAY[via], 7, near[7 - ONE_AWAY[via]], 1)
        for d, along in zip(ONE_AWAY, ON):
            pass_tokens(step, d, d + along, near[along], 1)

    slot = lax.broadcasted_iota(jnp.int32, (1, slots), 1)
    slot_core = slot // (CUBE * block)
    slot_chip = slot // block % CUBE
    slot_source = slot // MOST % CUBE
    slot_rank = slot % MOST
    pairs = [(coord, paired(coord, other)) for coord in place]
    chip = (
        jnp.where(slot_chip // 4 == 0, pairs[0][0], pairs[0][1]) * SIDE
        + jnp.where(slot_chip // 2 % 2 == 0, pairs[1][0], pairs[1][1])
    ) * SIDE + jnp.where(slot_chip % 2 == 0, pairs[2][0], pairs[2][1])
    slot_expert = chip * 2 + (core + slot_core) % 2
    widen = jnp.where(
        lax.broadcasted_iota(jnp.int32, (128, slots), 0) == slot_expert, 1.0, 0.0
    ).astype(BF16)

    wait_for(table.at[pl.ds(1, CUBE - 1)], table_sems.at[1])
    codes = jnp.concatenate([table[d, :count] for d in range(CUBE)], axis=0)
    weights = jnp.concatenate([table[d, count:] for d in range(CUBE)], axis=0)
    token_source = lax.broadcasted_iota(jnp.int32, (CUBE * count, 1), 0) // count
    hit = (dot(codes, widen) == (slot_rank + 1).astype(F32)) & (token_source == slot_source)
    mix[...] = jnp.where(hit, dot(weights, widen), 0.0).astype(BF16)
    pick[...] = jnp.where(hit, 1.0, 0.0).T.astype(BF16)

    def half_span(across):
        low = across * CUBE * block
        return pl.ds(low + block * (1 - across), CUBE * block - block * (1 - across))

    def send_rows(across, step):
        for d in ORDER + (0,) * across:
            span = pl.ds((across * CUBE + d) * block, block)
            send(
                sent.at[step, span], rows.at[step, span],
                (s2.at[0, across, step], s2.at[1, across, step]),
                far[d], other if across else core,
            )

    def select(step):
        wait_for(held.at[step, pl.ds(0, (len(ONE_AWAY) + 1) * count)], s1.at[1, 1, step])
        chosen_rows = dot(pick[...], held[step]).astype(BF16)
        sent[step] = chosen_rows
        rows[step, :block] = chosen_rows[:block]
        send_rows(0, step)
        for which in range(3):
            weight_send(which, step).start()

    def inward(step, carry):
        select(step)
        return carry

    lax.fori_loop(0, steps, inward, 0)

    def second_half(step, carry):
        send_rows(1, step)
        return carry

    lax.fori_loop(0, steps, second_half, 0)

    half = gate_v.shape[3]
    for across in range(2):
        low = across * CUBE * block
        these = slice(low, low + CUBE * block)

        def accumulate(step, carry):
            if across == 0:
                for which in range(2):
                    weight_load(which, step).wait()
                    weight_send(which, step).wait_recv()
            wait_for(rows.at[step, half_span(across)], s2.at[1, across, step])
            arrived = rows[step, these]
            for h in range(2):
                gate_acc[these, h * half : (h + 1) * half] += dot(arrived, gate_v[step, h])
                up_acc[these, h * half : (h + 1) * half] += dot(arrived, up_v[step, h])
            return carry

        lax.fori_loop(0, steps, accumulate, 0)
        gate = gate_acc[these]
        hidden[these] = (gate / (1.0 + jnp.exp(-gate)) * up_acc[these]).astype(BF16)

        def project(step, carry):
            if across == 0:
                weight_load(2, step).wait()
                weight_send(2, step).wait_recv()
            result = (
                dot_t(hidden[these, :half], down_v[step, 0])
                + dot_t(hidden[these, half:], down_v[step, 1])
            ).astype(BF16)
            made[step, these] = result
            if across == 0:
                back[step, :block] = result[:block]
            for d in ORDER + (0,) * across:
                span = pl.ds((across * CUBE + d) * block, block)
                send(
                    made.at[step, span], back.at[step, span],
                    (s3.at[0, across, step], s3.at[1, across, step]),
                    near[d] if across else far[d], other if across else core,
                )
            return carry

        lax.fori_loop(0, steps, project, 0)

    def pass_sums(source, step, block_here, block_there, chip, phase):
        send(
            source.at[step, pl.ds(block_here * count, count)],
            last.at[step, pl.ds(block_there * count, count)],
            (s4.at[0, phase, step], s4.at[1, phase, step]), chip, core,
        )

    def combine(step, carry):
        for across in range(2):
            wait_for(back.at[step, half_span(across)], s3.at[1, across, step])
        sums = dot(mix[...], back[step]).astype(BF16)
        part[step] = sums
        via = lax.rem(step, len(ONE_AWAY))
        pass_sums(part, step, 7, 7, jnp.where(via == 0, near[6], jnp.where(via == 1, near[5], near[3])), 0)
        for d, along in zip(ONE_AWAY, ON):
            pass_sums(part, step, d + along, d + along, near[along], 0)
        return carry

    def relay(step, carry):
        wait_for(last.at[step, pl.ds(0, (len(ONE_AWAY) + 1) * count)], s4.at[1, 0, step])
        via = lax.rem(step, len(ONE_AWAY))
        farthest = last[step, 7 * count :].astype(F32)
        for k, (d, along) in enumerate(zip(ONE_AWAY, ON)):
            here = pl.ds(d * count, count)
            total = part[step, here].astype(F32) + last[step, pl.ds((d + along) * count, count)].astype(F32)
            moved[step, here] = (total + jnp.where(via == k, farthest, 0.0)).astype(BF16)
        for d in ONE_AWAY:
            pass_sums(moved, step, d, d, near[d], 1)
        return carry

    def finish(step, carry):
        wait_for(last.at[step, pl.ds(0, len(ONE_AWAY) * count)], s4.at[1, 1, step])
        total = part[step, :count].astype(F32)
        for d in ONE_AWAY:
            total = total + last[step, d * count : (d + 1) * count].astype(F32)
        out[:, feature_span(step)] = total.astype(BF16)
        return carry

    lax.fori_loop(0, steps, combine, 0)
    lax.fori_loop(0, steps, relay, 0)
    lax.fori_loop(0, steps, finish, 0)

    wait_for(table.at[pl.ds(1, CUBE - 1)], table_sems.at[0])

    def drain(step, carry):
        for phase in range(2):
            moved_rows = pl.ds(0, (len(ONE_AWAY) + 1 - phase) * count)
            wait_for(held.at[step, pl.ds(0, (len(ONE_AWAY) + phase) * count)], s1.at[0, phase, step])
            wait_for(part.at[step, moved_rows], s4.at[0, phase, step])
        for across in range(2):
            wait_for(sent.at[step, half_span(across)], s2.at[0, across, step])
            wait_for(made.at[step, half_span(across)], s3.at[0, across, step])
        for which in range(3):
            weight_send(which, step).wait_send()
        return carry

    lax.fori_loop(0, steps, drain, 0)


def body(tokens, gate_weights, expert_ids, w_gate, w_up, w_down):
    count, features = tokens.shape
    units = w_gate.shape[2]
    steps = features // STEP
    gathered = CUBE * count
    slots = 2 * CUBE * CUBE * MOST
    dma = pltpu.SemaphoreType.DMA
    whole = pl.BlockSpec(memory_space=pl.ANY)
    vmem = pl.BlockSpec(memory_space=pltpu.VMEM)
    return pl.pallas_call(
        kernel,
        out_shape=jax.ShapeDtypeStruct((count, features), BF16),
        in_specs=[whole, vmem, vmem, whole, whole, whole],
        out_specs=vmem,
        scratch_shapes=[
            pltpu.VMEM((steps, gathered, STEP), BF16),
            pltpu.VMEM((CUBE, 2 * count, 128), BF16),
            pltpu.VMEM((slots, gathered), BF16),
            pltpu.VMEM((gathered, slots), BF16),
            pltpu.VMEM((steps, slots, STEP), BF16),
            pltpu.VMEM((steps, slots, STEP), BF16),
            pltpu.VMEM((slots, 2 * units), F32),
            pltpu.VMEM((slots, 2 * units), F32),
            pltpu.VMEM((slots, 2 * units), BF16),
            pltpu.VMEM((steps, slots, STEP), BF16),
            pltpu.VMEM((steps, slots, STEP), BF16),
            pltpu.VMEM((steps, gathered, STEP), BF16),
            pltpu.VMEM((steps, gathered, STEP), BF16),
            pltpu.VMEM((steps, gathered, STEP), BF16),
            pltpu.VMEM((steps, 2, STEP, units), BF16),
            pltpu.VMEM((steps, 2, STEP, units), BF16),
            pltpu.VMEM((steps, 2, STEP, units), BF16),
            dma((steps,)),
            dma((2,)),
            dma((2, 2, steps)),
            dma((2, 2, steps)),
            dma((2, 2, steps)),
            dma((2, 2, steps)),
            dma((3, steps)),
            dma((3, steps)),
            dma((3, steps)),
        ],
        compiler_params=pltpu.CompilerParams(
            collective_id=0, has_side_effects=True, vmem_limit_bytes=66_000_000
        ),
    )(tokens, gate_weights.T, expert_ids.T, w_gate, w_up, w_down)


def solution(mesh):
    placed = (
        P(("grp", "loc"), None),
        P(("grp", "loc"), None),
        P(("grp", "loc"), None),
        P("grp", None, "loc"),
        P("grp", None, "loc"),
        P("grp", None, "loc"),
    )
    return jax.shard_map(
        body, mesh=mesh, in_specs=placed, out_specs=P(("grp", "loc"), None), check_vma=False
    )
```

```python
import jax
import jax.numpy as jnp
from jax import lax
from jax.experimental import pallas as pl
from jax.experimental.pallas import tpu as pltpu
from jax.sharding import PartitionSpec as P

SIDE = 4
CUBE = 8
MOST = 4
STEP = 896
ORDER = (7, 3, 5, 6, 1, 2, 4)
ONE_AWAY = (1, 2, 4)
ON = (2, 4, 1)
F32 = jnp.float32
BF16 = jnp.bfloat16


def paired(coord, kind):
    odd = lax.rem(coord + kind, 2)
    return lax.rem(coord + SIDE + 1 - 2 * odd, SIDE)


def cube_of(place, kind):
    pairs = [(coord, paired(coord, kind)) for coord in place]
    return [
        (pairs[0][d // 4] * SIDE + pairs[1][d // 2 % 2]) * SIDE + pairs[2][d % 2]
        for d in range(CUBE)
    ]


def dot(left, right):
    return jnp.dot(left, right, preferred_element_type=F32)


def dot_t(left, right):
    return lax.dot_general(left, right, (((1,), (1,)), ((), ())), preferred_element_type=F32)


def kernel(
    tokens, scales_in, ids_in, w_gate, w_up, w_down, out,
    held, table, pick, mix, sent, rows, gate_acc, up_acc, hidden, made, back, part, last, moved,
    gate_v, up_v, down_v, scales, ids, small_sem,
    tok_sem, table_sems, s1, s2, s3, s4, w_local, w_send, w_recv,
):
    count = tokens.shape[0]
    steps = held.shape[0]
    block = CUBE * MOST
    slots = 2 * CUBE * block
    me = lax.axis_index("grp")
    core = lax.axis_index("loc")
    other = 1 - core
    place = (me // (SIDE * SIDE), lax.rem(me // SIDE, SIDE), lax.rem(me, SIDE))
    near = cube_of(place, core)
    far = cube_of(place, other)

    def feature_span(step):
        return pl.ds(pl.multiple_of(step * STEP, STEP), STEP)

    def token_load(step):
        return pltpu.make_async_copy(
            tokens.at[:, feature_span(step)], held.at[step, pl.ds(0, count)], tok_sem.at[step]
        )

    def weight_load(which, step):
        source = (w_gate, w_up, w_down)[which]
        target = (gate_v, up_v, down_v)[which]
        return pltpu.make_async_copy(
            source.at[core, feature_span(step)], target.at[step, 0], w_local.at[which, step]
        )

    def weight_send(which, step):
        source = (w_gate, w_up, w_down)[which]
        target = (gate_v, up_v, down_v)[which]
        return pltpu.make_async_remote_copy(
            src_ref=source.at[other, feature_span(step)],
            dst_ref=target.at[step, 1],
            send_sem=w_send.at[which, step],
            recv_sem=w_recv.at[which, step],
            device_id={"grp": me, "loc": other},
            device_id_type=pl.DeviceIdType.MESH,
        )

    def send(source, target, sems, chip, to_core):
        pltpu.make_async_remote_copy(
            src_ref=source,
            dst_ref=target,
            send_sem=sems[0],
            recv_sem=sems[1],
            device_id={"grp": chip, "loc": to_core},
            device_id_type=pl.DeviceIdType.MESH,
        ).start()

    def wait_for(ref, sem):
        pltpu.make_async_copy(ref, ref, sem).wait()

    def pass_tokens(step, block_here, block_there, chip, phase):
        send(
            held.at[step, pl.ds(block_here * count, count)],
            held.at[step, pl.ds(block_there * count, count)],
            (s1.at[0, phase, step], s1.at[1, phase, step]), chip, core,
        )

    for step in range(steps):
        token_load(step).start()
    small_loads = [
        pltpu.make_async_copy(ids_in, ids, small_sem.at[0]),
        pltpu.make_async_copy(scales_in, scales, small_sem.at[1]),
    ]
    for load in small_loads:
        load.start()
    barrier = pltpu.get_barrier_semaphore()
    partners = [(me, other)]
    for d in range(1, CUBE):
        partners += [(near[d], core), (near[d], other), (far[d], core), (far[d], other)]
    for chip, to_core in partners:
        pl.semaphore_signal(
            barrier, inc=1, device_id={"grp": chip, "loc": to_core},
            device_id_type=pl.DeviceIdType.MESH,
        )

    def start_weights(step, carry):
        for which in range(3):
            weight_load(which, step).start()
        return carry

    lax.fori_loop(0, steps, start_weights, 0)

    for load in small_loads:
        load.wait()
    expert_row = lax.broadcasted_iota(jnp.int32, (128, count), 0)
    chosen = jnp.zeros((128, count), F32)
    weight_of = jnp.zeros((128, count), F32)
    for k in range(ids.shape[0]):
        match = ids[k : k + 1, :] == expert_row
        chosen = chosen + jnp.where(match, 1.0, 0.0)
        weight_of = weight_of + jnp.where(match, scales[k : k + 1, :].astype(F32), 0.0)
    column = lax.broadcasted_iota(jnp.int32, (count, count), 1)
    row = lax.broadcasted_iota(jnp.int32, (count, count), 0)
    same = jnp.where(column == row, 1.0, 0.0).astype(BF16)
    before = jnp.where(column < row, 1.0, 0.0).astype(BF16)
    chosen = chosen.astype(BF16)
    table[0, :count] = (dot_t(same, chosen) * (dot_t(before, chosen) + 1.0)).astype(BF16)
    table[0, count:] = dot_t(same, weight_of.astype(BF16)).astype(BF16)
    gate_acc[...] = jnp.zeros_like(gate_acc)
    up_acc[...] = jnp.zeros_like(up_acc)

    pl.semaphore_wait(barrier, len(partners))

    for step in range(steps):
        token_load(step).wait()
        for d in ONE_AWAY:
            pass_tokens(step, 0, d, near[d], 0)
        if step == 0:
            for d in ORDER:
                send(table.at[0], table.at[d], (table_sems.at[0], table_sems.at[1]), near[d], core)

    for step in range(steps):
        wait_for(held.at[step, pl.ds(0, len(ONE_AWAY) * count)], s1.at[1, 0, step])
        via = step % len(ONE_AWAY)
        pass_tokens(step, ONE_AWAY[via], 7, near[7 - ONE_AWAY[via]], 1)
        for d, along in zip(ONE_AWAY, ON):
            pass_tokens(step, d, d + along, near[along], 1)

    slot = lax.broadcasted_iota(jnp.int32, (1, slots), 1)
    slot_core = slot // (CUBE * block)
    slot_chip = slot // block % CUBE
    slot_source = slot // MOST % CUBE
    slot_rank = slot % MOST
    pairs = [(coord, paired(coord, other)) for coord in place]
    chip = (
        jnp.where(slot_chip // 4 == 0, pairs[0][0], pairs[0][1]) * SIDE
        + jnp.where(slot_chip // 2 % 2 == 0, pairs[1][0], pairs[1][1])
    ) * SIDE + jnp.where(slot_chip % 2 == 0, pairs[2][0], pairs[2][1])
    slot_expert = chip * 2 + (core + slot_core) % 2
    widen = jnp.where(
        lax.broadcasted_iota(jnp.int32, (128, slots), 0) == slot_expert, 1.0, 0.0
    ).astype(BF16)

    wait_for(table.at[pl.ds(1, CUBE - 1)], table_sems.at[1])
    codes = jnp.concatenate([table[d, :count] for d in range(CUBE)], axis=0)
    weights = jnp.concatenate([table[d, count:] for d in range(CUBE)], axis=0)
    token_source = lax.broadcasted_iota(jnp.int32, (CUBE * count, 1), 0) // count
    hit = (dot(codes, widen) == (slot_rank + 1).astype(F32)) & (token_source == slot_source)
    mix[...] = jnp.where(hit, dot(weights, widen), 0.0).astype(BF16)
    pick[...] = jnp.where(hit, 1.0, 0.0).T.astype(BF16)

    def half_span(across):
        low = across * CUBE * block
        return pl.ds(low + block * (1 - across), CUBE * block - block * (1 - across))

    def send_rows(across, step):
        for d in ORDER + (0,) * across:
            span = pl.ds((across * CUBE + d) * block, block)
            send(
                sent.at[step, span], rows.at[step, span],
                (s2.at[0, across, step], s2.at[1, across, step]),
                far[d], other if across else core,
            )

    def select(step):
        wait_for(held.at[step, pl.ds(0, (len(ONE_AWAY) + 1) * count)], s1.at[1, 1, step])
        chosen_rows = dot(pick[...], held[step]).astype(BF16)
        sent[step] = chosen_rows
        rows[step, :block] = chosen_rows[:block]
        send_rows(0, step)
        for which in range(3):
            weight_send(which, step).start()

    def inward(step, carry):
        select(step)
        return carry

    lax.fori_loop(0, steps, inward, 0)

    def second_half(step, carry):
        send_rows(1, step)
        return carry

    lax.fori_loop(0, steps, second_half, 0)

    half = gate_v.shape[3]
    for across in range(2):
        low = across * CUBE * block
        these = slice(low, low + CUBE * block)

        def accumulate(step, carry):
            if across == 0:
                for which in range(2):
                    weight_load(which, step).wait()
                    weight_send(which, step).wait_recv()
            wait_for(rows.at[step, half_span(across)], s2.at[1, across, step])
            arrived = rows[step, these]
            for h in range(2):
                gate_acc[these, h * half : (h + 1) * half] += dot(arrived, gate_v[step, h])
                up_acc[these, h * half : (h + 1) * half] += dot(arrived, up_v[step, h])
            return carry

        lax.fori_loop(0, steps, accumulate, 0)
        gate = gate_acc[these]
        hidden[these] = (gate / (1.0 + jnp.exp(-gate)) * up_acc[these]).astype(BF16)

        def project(step, carry):
            if across == 0:
                weight_load(2, step).wait()
                weight_send(2, step).wait_recv()
            result = (
                dot_t(hidden[these, :half], down_v[step, 0])
                + dot_t(hidden[these, half:], down_v[step, 1])
            ).astype(BF16)
            made[step, these] = result
            if across == 0:
                back[step, :block] = result[:block]
            for d in ORDER + (0,) * across:
                span = pl.ds((across * CUBE + d) * block, block)
                send(
                    made.at[step, span], back.at[step, span],
                    (s3.at[0, across, step], s3.at[1, across, step]),
                    near[d] if across else far[d], other if across else core,
                )
            return carry

        lax.fori_loop(0, steps, project, 0)

    def pass_sums(source, step, block_here, block_there, chip, phase):
        send(
            source.at[step, pl.ds(block_here * count, count)],
            last.at[step, pl.ds(block_there * count, count)],
            (s4.at[0, phase, step], s4.at[1, phase, step]), chip, core,
        )

    def combine(step, carry):
        for across in range(2):
            wait_for(back.at[step, half_span(across)], s3.at[1, across, step])
        sums = dot(mix[...], back[step]).astype(BF16)
        part[step] = sums
        via = lax.rem(step, len(ONE_AWAY))
        pass_sums(part, step, 7, 7, jnp.where(via == 0, near[6], jnp.where(via == 1, near[5], near[3])), 0)
        for d, along in zip(ONE_AWAY, ON):
            pass_sums(part, step, d + along, d + along, near[along], 0)
        return carry

    def relay(step, carry):
        wait_for(last.at[step, pl.ds(0, (len(ONE_AWAY) + 1) * count)], s4.at[1, 0, step])
        via = lax.rem(step, len(ONE_AWAY))
        farthest = last[step, 7 * count :].astype(F32)
        for k, (d, along) in enumerate(zip(ONE_AWAY, ON)):
            here = pl.ds(d * count, count)
            total = part[step, here].astype(F32) + last[step, pl.ds((d + along) * count, count)].astype(F32)
            moved[step, here] = (total + jnp.where(via == k, farthest, 0.0)).astype(BF16)
        for d in ONE_AWAY:
            pass_sums(moved, step, d, d, near[d], 1)
        return carry

    def finish(step, carry):
        wait_for(last.at[step, pl.ds(0, len(ONE_AWAY) * count)], s4.at[1, 1, step])
        total = part[step, :count].astype(F32)
        for d in ONE_AWAY:
            total = total + last[step, d * count : (d + 1) * count].astype(F32)
        out[:, feature_span(step)] = total.astype(BF16)
        return carry

    lax.fori_loop(0, steps, combine, 0)
    lax.fori_loop(0, steps, relay, 0)
    lax.fori_loop(0, steps, finish, 0)

    wait_for(table.at[pl.ds(1, CUBE - 1)], table_sems.at[0])

    def drain(step, carry):
        for phase in range(2):
            moved_rows = pl.ds(0, (len(ONE_AWAY) + 1 - phase) * count)
            wait_for(held.at[step, pl.ds(0, (len(ONE_AWAY) + phase) * count)], s1.at[0, phase, step])
            wait_for(part.at[step, moved_rows], s4.at[0, phase, step])
        for across in range(2):
            wait_for(sent.at[step, half_span(across)], s2.at[0, across, step])
            wait_for(made.at[step, half_span(across)], s3.at[0, across, step])
        for which in range(3):
            weight_send(which, step).wait_send()
        return carry

    lax.fori_loop(0, steps, drain, 0)


def body(tokens, gate_weights, expert_ids, w_gate, w_up, w_down):
    count, features = tokens.shape
    choices = expert_ids.shape[1]
    units = w_gate.shape[2]
    steps = features // STEP
    gathered = CUBE * count
    slots = 2 * CUBE * CUBE * MOST
    dma = pltpu.SemaphoreType.DMA
    whole = pl.BlockSpec(memory_space=pl.ANY)
    vmem = pl.BlockSpec(memory_space=pltpu.VMEM)
    return pl.pallas_call(
        kernel,
        out_shape=pltpu.VMEM((count, features), BF16),
        in_specs=[whole, whole, whole, whole, whole, whole],
        out_specs=vmem,
        scratch_shapes=[
            pltpu.VMEM((steps, gathered, STEP), BF16),
            pltpu.VMEM((CUBE, 2 * count, 128), BF16),
            pltpu.VMEM((slots, gathered), BF16),
            pltpu.VMEM((gathered, slots), BF16),
            pltpu.VMEM((steps, slots, STEP), BF16),
            pltpu.VMEM((steps, slots, STEP), BF16),
            pltpu.VMEM((slots, 2 * units), F32),
            pltpu.VMEM((slots, 2 * units), F32),
            pltpu.VMEM((slots, 2 * units), BF16),
            pltpu.VMEM((steps, slots, STEP), BF16),
            pltpu.VMEM((steps, slots, STEP), BF16),
            pltpu.VMEM((steps, gathered, STEP), BF16),
            pltpu.VMEM((steps, gathered, STEP), BF16),
            pltpu.VMEM((steps, gathered, STEP), BF16),
            pltpu.VMEM((steps, 2, STEP, units), BF16),
            pltpu.VMEM((steps, 2, STEP, units), BF16),
            pltpu.VMEM((steps, 2, STEP, units), BF16),
            pltpu.VMEM((choices, count), BF16),
            pltpu.VMEM((choices, count), jnp.int32),
            dma((2,)),
            dma((steps,)),
            dma((2,)),
            dma((2, 2, steps)),
            dma((2, 2, steps)),
            dma((2, 2, steps)),
            dma((2, 2, steps)),
            dma((3, steps)),
            dma((3, steps)),
            dma((3, steps)),
        ],
        compiler_params=pltpu.CompilerParams(
            collective_id=0, has_side_effects=True, vmem_limit_bytes=54_000_000
        ),
    )(*(pltpu.with_memory_space_constraint(x, pltpu.HBM) for x in (tokens, gate_weights.T, expert_ids.T, w_gate, w_up, w_down)))


def solution(mesh):
    placed = (
        P(("grp", "loc"), None),
        P(("grp", "loc"), None),
        P(("grp", "loc"), None),
        P("grp", None, "loc"),
        P("grp", None, "loc"),
        P("grp", None, "loc"),
    )
    return jax.shard_map(
        body, mesh=mesh, in_specs=placed, out_specs=P(("grp", "loc"), None), check_vma=False
    )
```

```python
import jax
import jax.numpy as jnp
from jax import lax
from jax.experimental import pallas as pl
from jax.experimental.pallas import tpu as pltpu
from jax.sharding import PartitionSpec as P

SIDE = 4
CUBE = 8
MOST = 4
STEP = 896
ORDER = (7, 3, 5, 6, 1, 2, 4)
ONE_AWAY = (1, 2, 4)
ON = (2, 4, 1)
F32 = jnp.float32
BF16 = jnp.bfloat16


def paired(coord, kind):
    odd = lax.rem(coord + kind, 2)
    return lax.rem(coord + SIDE + 1 - 2 * odd, SIDE)


def cube_of(place, kind):
    pairs = [(coord, paired(coord, kind)) for coord in place]
    return [
        (pairs[0][d // 4] * SIDE + pairs[1][d // 2 % 2]) * SIDE + pairs[2][d % 2]
        for d in range(CUBE)
    ]


def dot(left, right):
    return jnp.dot(left, right, preferred_element_type=F32)


def dot_t(left, right):
    return lax.dot_general(left, right, (((1,), (1,)), ((), ())), preferred_element_type=F32)


def kernel(
    tokens, scales_in, ids_in, w_gate, w_up, w_down, out,
    held, table, pick, mix, sent, rows, gate_acc, up_acc, hidden, made, back, part, last, moved,
    gate_v, up_v, down_v, scales, ids, ready, small_sem,
    tok_sem, table_sems, s1, s2, s3, s4, w_local, w_send, w_recv,
):
    count = tokens.shape[0]
    steps = held.shape[0]
    block = CUBE * MOST
    slots = 2 * CUBE * block
    me = lax.axis_index("grp")
    core = lax.axis_index("loc")
    other = 1 - core
    place = (me // (SIDE * SIDE), lax.rem(me // SIDE, SIDE), lax.rem(me, SIDE))
    near = cube_of(place, core)
    far = cube_of(place, other)

    def feature_span(step):
        return pl.ds(pl.multiple_of(step * STEP, STEP), STEP)

    def token_load(step):
        return pltpu.make_async_copy(
            tokens.at[:, feature_span(step)], held.at[step, pl.ds(0, count)], tok_sem.at[step]
        )

    def weight_load(which, step):
        source = (w_gate, w_up, w_down)[which]
        target = (gate_v, up_v, down_v)[which]
        return pltpu.make_async_copy(
            source.at[core, feature_span(step)], target.at[step, 0], w_local.at[which, step]
        )

    def weight_send(which, step):
        source = (w_gate, w_up, w_down)[which]
        target = (gate_v, up_v, down_v)[which]
        return pltpu.make_async_remote_copy(
            src_ref=source.at[other, feature_span(step)],
            dst_ref=target.at[step, 1],
            send_sem=w_send.at[which, step],
            recv_sem=w_recv.at[which, step],
            device_id={"grp": me, "loc": other},
            device_id_type=pl.DeviceIdType.MESH,
        )

    def send(source, target, sems, chip, to_core):
        pltpu.make_async_remote_copy(
            src_ref=source,
            dst_ref=target,
            send_sem=sems[0],
            recv_sem=sems[1],
            device_id={"grp": chip, "loc": to_core},
            device_id_type=pl.DeviceIdType.MESH,
        ).start()

    def wait_for(ref, sem):
        pltpu.make_async_copy(ref, ref, sem).wait()

    def pass_tokens(step, block_here, block_there, chip, phase):
        send(
            held.at[step, pl.ds(block_here * count, count)],
            held.at[step, pl.ds(block_there * count, count)],
            (s1.at[0, phase, step], s1.at[1, phase, step]), chip, core,
        )

    for step in range(steps):
        token_load(step).start()
    small_loads = [
        pltpu.make_async_copy(ids_in, ids, small_sem.at[0]),
        pltpu.make_async_copy(scales_in, scales, small_sem.at[1]),
    ]
    for load in small_loads:
        load.start()
    neighbours = [(me, other)] + [(cube[d], core) for cube in (near, far) for d in ONE_AWAY]

    def greet(semaphore):
        for chip, to_core in neighbours:
            pl.semaphore_signal(
                semaphore, inc=1, device_id={"grp": chip, "loc": to_core},
                device_id_type=pl.DeviceIdType.MESH,
            )

    def greeted(semaphore):
        pl.semaphore_wait(semaphore, len(neighbours))

    barrier = pltpu.get_barrier_semaphore()
    greet(barrier)

    def start_weights(step, carry):
        for which in range(3):
            weight_load(which, step).start()
        return carry

    lax.fori_loop(0, steps, start_weights, 0)

    greeted(barrier)
    greet(ready.at[0])

    def pass_table(block_here, block_there, chip, phase):
        send(
            table.at[block_here], table.at[block_there],
            (table_sems.at[0, phase], table_sems.at[1, phase]), chip, core,
        )

    def pass_on(step):
        wait_for(held.at[step, pl.ds(0, len(ONE_AWAY) * count)], s1.at[1, 0, step])
        via = step % len(ONE_AWAY)
        pass_tokens(step, ONE_AWAY[via], 7, near[7 - ONE_AWAY[via]], 1)
        for d, along in zip(ONE_AWAY, ON):
            pass_tokens(step, d, d + along, near[along], 1)

    for step in range(steps):
        token_load(step).wait()
        for d in ONE_AWAY:
            pass_tokens(step, 0, d, near[d], 0)
    for load in small_loads:
        load.wait()
    expert_row = lax.broadcasted_iota(jnp.int32, (128, count), 0)
    chosen = jnp.zeros((128, count), F32)
    weight_of = jnp.zeros((128, count), F32)
    for k in range(ids.shape[0]):
        match = ids[k : k + 1, :] == expert_row
        chosen = chosen + jnp.where(match, 1.0, 0.0)
        weight_of = weight_of + jnp.where(match, scales[k : k + 1, :].astype(F32), 0.0)
    column = lax.broadcasted_iota(jnp.int32, (count, count), 1)
    row = lax.broadcasted_iota(jnp.int32, (count, count), 0)
    same = jnp.where(column == row, 1.0, 0.0).astype(BF16)
    before = jnp.where(column < row, 1.0, 0.0).astype(BF16)
    chosen = chosen.astype(BF16)
    table[0, :count] = (dot_t(same, chosen) * (dot_t(before, chosen) + 1.0)).astype(BF16)
    table[0, count:] = dot_t(same, weight_of.astype(BF16)).astype(BF16)
    gate_acc[...] = jnp.zeros_like(gate_acc)
    up_acc[...] = jnp.zeros_like(up_acc)

    for d in ONE_AWAY:
        pass_table(0, d, near[d], 0)
    greeted(ready.at[0])
    greet(ready.at[1])
    pass_on(0)
    pass_on(1)
    wait_for(table.at[pl.ds(0, len(ONE_AWAY))], table_sems.at[1, 0])
    pass_table(1, 7, near[6], 1)
    for d, along in zip(ONE_AWAY, ON):
        pass_table(d, d + along, near[along], 1)
    greeted(ready.at[1])
    greet(ready.at[2])
    for step in range(2, steps):
        pass_on(step)

    slot = lax.broadcasted_iota(jnp.int32, (1, slots), 1)
    slot_core = slot // (CUBE * block)
    slot_chip = slot // block % CUBE
    slot_source = slot // MOST % CUBE
    slot_rank = slot % MOST
    pairs = [(coord, paired(coord, other)) for coord in place]
    chip = (
        jnp.where(slot_chip // 4 == 0, pairs[0][0], pairs[0][1]) * SIDE
        + jnp.where(slot_chip // 2 % 2 == 0, pairs[1][0], pairs[1][1])
    ) * SIDE + jnp.where(slot_chip % 2 == 0, pairs[2][0], pairs[2][1])
    slot_expert = chip * 2 + (core + slot_core) % 2
    widen = jnp.where(
        lax.broadcasted_iota(jnp.int32, (128, slots), 0) == slot_expert, 1.0, 0.0
    ).astype(BF16)

    wait_for(table.at[pl.ds(0, len(ONE_AWAY) + 1)], table_sems.at[1, 1])
    codes = jnp.concatenate([table[d, :count] for d in range(CUBE)], axis=0)
    weights = jnp.concatenate([table[d, count:] for d in range(CUBE)], axis=0)
    token_source = lax.broadcasted_iota(jnp.int32, (CUBE * count, 1), 0) // count
    hit = (dot(codes, widen) == (slot_rank + 1).astype(F32)) & (token_source == slot_source)
    mix[...] = jnp.where(hit, dot(weights, widen), 0.0).astype(BF16)
    pick[...] = jnp.where(hit, 1.0, 0.0).T.astype(BF16)

    greeted(ready.at[2])

    def half_span(across):
        low = across * CUBE * block
        return pl.ds(low + block * (1 - across), CUBE * block - block * (1 - across))

    def send_rows(across, step):
        for d in ORDER + (0,) * across:
            span = pl.ds((across * CUBE + d) * block, block)
            send(
                sent.at[step, span], rows.at[step, span],
                (s2.at[0, across, step], s2.at[1, across, step]),
                far[d], other if across else core,
            )

    def select(step):
        wait_for(held.at[step, pl.ds(0, (len(ONE_AWAY) + 1) * count)], s1.at[1, 1, step])
        chosen_rows = dot(pick[...], held[step]).astype(BF16)
        sent[step] = chosen_rows
        rows[step, :block] = chosen_rows[:block]
        send_rows(0, step)
        for which in range(3):
            weight_send(which, step).start()

    def inward(step, carry):
        select(step)
        return carry

    lax.fori_loop(0, steps, inward, 0)

    def second_half(step, carry):
        send_rows(1, step)
        return carry

    lax.fori_loop(0, steps, second_half, 0)

    half = gate_v.shape[3]
    for across in range(2):
        low = across * CUBE * block
        these = slice(low, low + CUBE * block)

        def accumulate(step, carry):
            if across == 0:
                for which in range(2):
                    weight_load(which, step).wait()
                    weight_send(which, step).wait_recv()
            wait_for(rows.at[step, half_span(across)], s2.at[1, across, step])
            arrived = rows[step, these]
            for h in range(2):
                gate_acc[these, h * half : (h + 1) * half] += dot(arrived, gate_v[step, h])
                up_acc[these, h * half : (h + 1) * half] += dot(arrived, up_v[step, h])
            return carry

        lax.fori_loop(0, steps, accumulate, 0)
        gate = gate_acc[these]
        hidden[these] = (gate / (1.0 + jnp.exp(-gate)) * up_acc[these]).astype(BF16)

        def project(step, carry):
            if across == 0:
                weight_load(2, step).wait()
                weight_send(2, step).wait_recv()
            result = (
                dot_t(hidden[these, :half], down_v[step, 0])
                + dot_t(hidden[these, half:], down_v[step, 1])
            ).astype(BF16)
            made[step, these] = result
            if across == 0:
                back[step, :block] = result[:block]
            for d in ORDER + (0,) * across:
                span = pl.ds((across * CUBE + d) * block, block)
                send(
                    made.at[step, span], back.at[step, span],
                    (s3.at[0, across, step], s3.at[1, across, step]),
                    near[d] if across else far[d], other if across else core,
                )
            return carry

        lax.fori_loop(0, steps, project, 0)

    def pass_sums(source, step, block_here, block_there, chip, phase):
        send(
            source.at[step, pl.ds(block_here * count, count)],
            last.at[step, pl.ds(block_there * count, count)],
            (s4.at[0, phase, step], s4.at[1, phase, step]), chip, core,
        )

    def combine(step, carry):
        for across in range(2):
            wait_for(back.at[step, half_span(across)], s3.at[1, across, step])
        sums = dot(mix[...], back[step]).astype(BF16)
        part[step] = sums
        via = lax.rem(step, len(ONE_AWAY))
        pass_sums(part, step, 7, 7, jnp.where(via == 0, near[6], jnp.where(via == 1, near[5], near[3])), 0)
        for d, along in zip(ONE_AWAY, ON):
            pass_sums(part, step, d + along, d + along, near[along], 0)
        return carry

    def relay(step, carry):
        wait_for(last.at[step, pl.ds(0, (len(ONE_AWAY) + 1) * count)], s4.at[1, 0, step])
        via = lax.rem(step, len(ONE_AWAY))
        farthest = last[step, 7 * count :].astype(F32)
        for k, (d, along) in enumerate(zip(ONE_AWAY, ON)):
            here = pl.ds(d * count, count)
            total = part[step, here].astype(F32) + last[step, pl.ds((d + along) * count, count)].astype(F32)
            moved[step, here] = (total + jnp.where(via == k, farthest, 0.0)).astype(BF16)
        for d in ONE_AWAY:
            pass_sums(moved, step, d, d, near[d], 1)
        return carry

    def finish(step, carry):
        wait_for(last.at[step, pl.ds(0, len(ONE_AWAY) * count)], s4.at[1, 1, step])
        total = part[step, :count].astype(F32)
        for d in ONE_AWAY:
            total = total + last[step, d * count : (d + 1) * count].astype(F32)
        out[:, feature_span(step)] = total.astype(BF16)
        return carry

    lax.fori_loop(0, steps, combine, 0)
    lax.fori_loop(0, steps, relay, 0)
    lax.fori_loop(0, steps, finish, 0)

    for phase in range(2):
        wait_for(table.at[pl.ds(0, len(ONE_AWAY) + phase)], table_sems.at[0, phase])

    def drain(step, carry):
        for phase in range(2):
            moved_rows = pl.ds(0, (len(ONE_AWAY) + 1 - phase) * count)
            wait_for(held.at[step, pl.ds(0, (len(ONE_AWAY) + phase) * count)], s1.at[0, phase, step])
            wait_for(part.at[step, moved_rows], s4.at[0, phase, step])
        for across in range(2):
            wait_for(sent.at[step, half_span(across)], s2.at[0, across, step])
            wait_for(made.at[step, half_span(across)], s3.at[0, across, step])
        for which in range(3):
            weight_send(which, step).wait_send()
        return carry

    lax.fori_loop(0, steps, drain, 0)


def body(tokens, gate_weights, expert_ids, w_gate, w_up, w_down):
    count, features = tokens.shape
    choices = expert_ids.shape[1]
    units = w_gate.shape[2]
    steps = features // STEP
    gathered = CUBE * count
    slots = 2 * CUBE * CUBE * MOST
    dma = pltpu.SemaphoreType.DMA
    whole = pl.BlockSpec(memory_space=pl.ANY)
    vmem = pl.BlockSpec(memory_space=pltpu.VMEM)
    return pl.pallas_call(
        kernel,
        out_shape=pltpu.VMEM((count, features), BF16),
        in_specs=[whole, whole, whole, whole, whole, whole],
        out_specs=vmem,
        scratch_shapes=[
            pltpu.VMEM((steps, gathered, STEP), BF16),
            pltpu.VMEM((CUBE, 2 * count, 128), BF16),
            pltpu.VMEM((slots, gathered), BF16),
            pltpu.VMEM((gathered, slots), BF16),
            pltpu.VMEM((steps, slots, STEP), BF16),
            pltpu.VMEM((steps, slots, STEP), BF16),
            pltpu.VMEM((slots, 2 * units), F32),
            pltpu.VMEM((slots, 2 * units), F32),
            pltpu.VMEM((slots, 2 * units), BF16),
            pltpu.VMEM((steps, slots, STEP), BF16),
            pltpu.VMEM((steps, slots, STEP), BF16),
            pltpu.VMEM((steps, gathered, STEP), BF16),
            pltpu.VMEM((steps, gathered, STEP), BF16),
            pltpu.VMEM((steps, gathered, STEP), BF16),
            pltpu.VMEM((steps, 2, STEP, units), BF16),
            pltpu.VMEM((steps, 2, STEP, units), BF16),
            pltpu.VMEM((steps, 2, STEP, units), BF16),
            pltpu.VMEM((choices, count), BF16),
            pltpu.VMEM((choices, count), jnp.int32),
            pltpu.SemaphoreType.REGULAR((3,)),
            dma((2,)),
            dma((steps,)),
            dma((2, 2)),
            dma((2, 2, steps)),
            dma((2, 2, steps)),
            dma((2, 2, steps)),
            dma((2, 2, steps)),
            dma((3, steps)),
            dma((3, steps)),
            dma((3, steps)),
        ],
        compiler_params=pltpu.CompilerParams(
            collective_id=0, has_side_effects=True, vmem_limit_bytes=54_000_000
        ),
    )(*(pltpu.with_memory_space_constraint(x, pltpu.HBM) for x in (tokens, gate_weights.T, expert_ids.T, w_gate, w_up, w_down)))


def solution(mesh):
    placed = (
        P(("grp", "loc"), None),
        P(("grp", "loc"), None),
        P(("grp", "loc"), None),
        P("grp", None, "loc"),
        P("grp", None, "loc"),
        P("grp", None, "loc"),
    )
    return jax.shard_map(
        body, mesh=mesh, in_specs=placed, out_specs=P(("grp", "loc"), None), check_vma=False
    )
```

```python
import jax
import jax.numpy as jnp
from jax import lax
from jax.experimental import pallas as pl
from jax.experimental.pallas import tpu as pltpu
from jax.sharding import PartitionSpec as P

SIDE = 4
CUBE = 8
MOST = 4
DIRECT = 1
STEP = 512
ORDER = (7, 3, 5, 6, 1, 2, 4)
ONE_AWAY = (1, 2, 4)
ON = (2, 4, 1)
F32 = jnp.float32
BF16 = jnp.bfloat16


def paired(coord, kind):
    odd = lax.rem(coord + kind, 2)
    return lax.rem(coord + SIDE + 1 - 2 * odd, SIDE)


def cube_of(place, kind):
    pairs = [(coord, paired(coord, kind)) for coord in place]
    return [
        (pairs[0][d // 4] * SIDE + pairs[1][d // 2 % 2]) * SIDE + pairs[2][d % 2]
        for d in range(CUBE)
    ]


def dot(left, right):
    return jnp.dot(left, right, preferred_element_type=F32)


def dot_t(left, right):
    return lax.dot_general(left, right, (((1,), (1,)), ((), ())), preferred_element_type=F32)


def kernel(
    tokens, scales_in, ids_in, w_gate, w_up, w_down, out,
    held, table, pick, mix, sent, rows, gate_acc, up_acc, hidden, made, back, part, last, moved,
    gate_v, up_v, down_v, scales, ids, ready, small_sem,
    tok_sem, table_sems, s1, s2, s3, s4, w_local, w_send, w_recv,
):
    count = tokens.shape[0]
    steps = held.shape[0]
    block = CUBE * MOST
    slots = 2 * CUBE * block
    me = lax.axis_index("grp")
    core = lax.axis_index("loc")
    other = 1 - core
    place = (me // (SIDE * SIDE), lax.rem(me // SIDE, SIDE), lax.rem(me, SIDE))
    near = cube_of(place, core)
    far = cube_of(place, other)

    def feature_span(step):
        return pl.ds(pl.multiple_of(step * STEP, STEP), STEP)

    def token_load(step):
        return pltpu.make_async_copy(
            tokens.at[:, feature_span(step)], held.at[step, pl.ds(0, count)], tok_sem.at[step]
        )

    def weight_load(which, step):
        source = (w_gate, w_up, w_down)[which]
        target = (gate_v, up_v, down_v)[which]
        return pltpu.make_async_copy(
            source.at[core, feature_span(step)], target.at[step, 0], w_local.at[which, step]
        )

    def weight_send(which, step):
        source = (w_gate, w_up, w_down)[which]
        target = (gate_v, up_v, down_v)[which]
        return pltpu.make_async_remote_copy(
            src_ref=source.at[other, feature_span(step)],
            dst_ref=target.at[step, 1],
            send_sem=w_send.at[which, step],
            recv_sem=w_recv.at[which, step],
            device_id={"grp": me, "loc": other},
            device_id_type=pl.DeviceIdType.MESH,
        )

    def send(source, target, sems, chip, to_core):
        pltpu.make_async_remote_copy(
            src_ref=source,
            dst_ref=target,
            send_sem=sems[0],
            recv_sem=sems[1],
            device_id={"grp": chip, "loc": to_core},
            device_id_type=pl.DeviceIdType.MESH,
        ).start()

    def wait_for(ref, sem):
        pltpu.make_async_copy(ref, ref, sem).wait()

    def pass_tokens(step, block_here, block_there, chip, phase):
        send(
            held.at[step, pl.ds(block_here * count, count)],
            held.at[step, pl.ds(block_there * count, count)],
            (s1.at[0, phase, step], s1.at[1, phase, step]), chip, core,
        )

    for step in range(steps):
        token_load(step).start()
    small_loads = [
        pltpu.make_async_copy(ids_in, ids, small_sem.at[0]),
        pltpu.make_async_copy(scales_in, scales, small_sem.at[1]),
    ]
    for load in small_loads:
        load.start()
    neighbours = [(me, other)] + [(cube[d], core) for cube in (near, far) for d in ONE_AWAY]

    def greet(semaphore):
        for chip, to_core in neighbours:
            pl.semaphore_signal(
                semaphore, inc=1, device_id={"grp": chip, "loc": to_core},
                device_id_type=pl.DeviceIdType.MESH,
            )

    def greeted(semaphore):
        pl.semaphore_wait(semaphore, len(neighbours))

    barrier = pltpu.get_barrier_semaphore()
    greet(barrier)


    greeted(barrier)
    greet(ready.at[0])

    def pass_table(block_here, block_there, chip, phase):
        send(
            table.at[block_here], table.at[block_there],
            (table_sems.at[0, phase], table_sems.at[1, phase]), chip, core,
        )

    def pass_on(step):
        wait_for(held.at[step, pl.ds(0, len(ONE_AWAY) * count)], s1.at[1, 0, step])
        via = step % len(ONE_AWAY)
        pass_tokens(step, ONE_AWAY[via], 7, near[7 - ONE_AWAY[via]], 1)
        for d, along in zip(ONE_AWAY, ON):
            pass_tokens(step, d, d + along, near[along], 1)

    for step in range(steps):
        token_load(step).wait()
        for d in ONE_AWAY:
            pass_tokens(step, 0, d, near[d], 0)
    def start_weights(step, carry):
        for which in range(3):
            weight_load(which, step).start()
        return carry

    lax.fori_loop(0, steps, start_weights, 0)

    for load in small_loads:
        load.wait()
    expert_row = lax.broadcasted_iota(jnp.int32, (128, count), 0)
    chosen = jnp.zeros((128, count), F32)
    weight_of = jnp.zeros((128, count), F32)
    for k in range(ids.shape[0]):
        match = ids[k : k + 1, :] == expert_row
        chosen = chosen + jnp.where(match, 1.0, 0.0)
        weight_of = weight_of + jnp.where(match, scales[k : k + 1, :].astype(F32), 0.0)
    column = lax.broadcasted_iota(jnp.int32, (count, count), 1)
    row = lax.broadcasted_iota(jnp.int32, (count, count), 0)
    same = jnp.where(column == row, 1.0, 0.0).astype(BF16)
    before = jnp.where(column < row, 1.0, 0.0).astype(BF16)
    chosen = chosen.astype(BF16)
    table[0, :count] = (dot_t(same, chosen) * (dot_t(before, chosen) + 1.0)).astype(BF16)
    table[0, count:] = dot_t(same, weight_of.astype(BF16)).astype(BF16)
    gate_acc[...] = jnp.zeros_like(gate_acc)
    up_acc[...] = jnp.zeros_like(up_acc)

    for d in ONE_AWAY:
        pass_table(0, d, near[d], 0)
    greeted(ready.at[0])
    greet(ready.at[1])
    pass_on(0)
    pass_on(1)
    wait_for(table.at[pl.ds(0, len(ONE_AWAY))], table_sems.at[1, 0])
    pass_table(1, 7, near[6], 1)
    for d, along in zip(ONE_AWAY, ON):
        pass_table(d, d + along, near[along], 1)
    greeted(ready.at[1])
    greet(ready.at[2])
    for step in range(2, steps):
        pass_on(step)

    slot = lax.broadcasted_iota(jnp.int32, (1, slots), 1)
    slot_core = slot // (CUBE * block)
    slot_chip = slot // block % CUBE
    slot_source = slot // MOST % CUBE
    slot_rank = slot % MOST
    pairs = [(coord, paired(coord, other)) for coord in place]
    chip = (
        jnp.where(slot_chip // 4 == 0, pairs[0][0], pairs[0][1]) * SIDE
        + jnp.where(slot_chip // 2 % 2 == 0, pairs[1][0], pairs[1][1])
    ) * SIDE + jnp.where(slot_chip % 2 == 0, pairs[2][0], pairs[2][1])
    slot_expert = chip * 2 + (core + slot_core) % 2
    widen = jnp.where(
        lax.broadcasted_iota(jnp.int32, (128, slots), 0) == slot_expert, 1.0, 0.0
    ).astype(BF16)

    wait_for(table.at[pl.ds(0, len(ONE_AWAY) + 1)], table_sems.at[1, 1])
    codes = jnp.concatenate([table[d, :count] for d in range(CUBE)], axis=0)
    weights = jnp.concatenate([table[d, count:] for d in range(CUBE)], axis=0)
    token_source = lax.broadcasted_iota(jnp.int32, (CUBE * count, 1), 0) // count
    hit = (dot(codes, widen) == (slot_rank + 1).astype(F32)) & (token_source == slot_source)
    mix[...] = jnp.where(hit, dot(weights, widen), 0.0).astype(BF16)
    pick[...] = jnp.where(hit, 1.0, 0.0).T.astype(BF16)

    greeted(ready.at[2])

    def half_span(across):
        low = across * CUBE * block
        return pl.ds(low + block * (1 - across), CUBE * block - block * (1 - across))

    def send_rows(across, step):
        for d in ORDER + (0,) * across:
            span = pl.ds((across * CUBE + d) * block, block)
            send(
                sent.at[step, span], rows.at[step, span],
                (s2.at[0, across, step], s2.at[1, across, step]),
                far[d], other if across else core,
            )

    def select(step):
        wait_for(held.at[step, pl.ds(0, (len(ONE_AWAY) + 1) * count)], s1.at[1, 1, step])
        chosen_rows = dot(pick[...], held[step]).astype(BF16)
        sent[step] = chosen_rows
        rows[step, :block] = chosen_rows[:block]
        send_rows(0, step)
        for which in range(3):
            weight_send(which, step).start()

    def inward(step, carry):
        select(step)
        return carry

    lax.fori_loop(0, steps, inward, 0)

    def second_half(step, carry):
        send_rows(1, step)
        return carry

    lax.fori_loop(0, steps, second_half, 0)

    half = gate_v.shape[3]
    for across in range(2):
        low = across * CUBE * block
        these = slice(low, low + CUBE * block)

        def accumulate(step, carry):
            if across == 0:
                for which in range(2):
                    weight_load(which, step).wait()
                    weight_send(which, step).wait_recv()
            wait_for(rows.at[step, half_span(across)], s2.at[1, across, step])
            arrived = rows[step, these]
            for h in range(2):
                gate_acc[these, h * half : (h + 1) * half] += dot(arrived, gate_v[step, h])
                up_acc[these, h * half : (h + 1) * half] += dot(arrived, up_v[step, h])
            return carry

        lax.fori_loop(0, steps, accumulate, 0)
        gate = gate_acc[these]
        hidden[these] = (gate / (1.0 + jnp.exp(-gate)) * up_acc[these]).astype(BF16)

        def project(step, carry):
            if across == 0:
                weight_load(2, step).wait()
                weight_send(2, step).wait_recv()
            result = (
                dot_t(hidden[these, :half], down_v[step, 0])
                + dot_t(hidden[these, half:], down_v[step, 1])
            ).astype(BF16)
            made[step, these] = result
            if across == 0:
                back[step, :block] = result[:block]
            for d in ORDER + (0,) * across:
                span = pl.ds((across * CUBE + d) * block, block)
                send(
                    made.at[step, span], back.at[step, span],
                    (s3.at[0, across, step], s3.at[1, across, step]),
                    near[d] if across else far[d], other if across else core,
                )
            return carry

        lax.fori_loop(0, steps, project, 0)

    relayed = steps - DIRECT

    def pass_sums(source, step, block_here, block_there, chip, phase):
        send(
            source.at[step, pl.ds(block_here * count, count)],
            last.at[step, pl.ds(block_there * count, count)],
            (s4.at[0, phase, step], s4.at[1, phase, step]), chip, core,
        )

    def combine(step, carry):
        for across in range(2):
            wait_for(back.at[step, half_span(across)], s3.at[1, across, step])
        sums = dot(mix[...], back[step]).astype(BF16)
        part[step] = sums
        via = lax.rem(step, len(ONE_AWAY))

        @pl.when(step < relayed)
        def _():
            corner = jnp.where(via == 0, near[6], jnp.where(via == 1, near[5], near[3]))
            pass_sums(part, step, 7, 7, corner, 0)
            for d, along in zip(ONE_AWAY, ON):
                pass_sums(part, step, d + along, d + along, near[along], 0)

        @pl.when(step >= relayed)
        def _():
            for d in ORDER:
                pass_sums(part, step, d, d, near[d], 0)

        return carry

    def relay(step, carry):
        wait_for(last.at[step, pl.ds(0, (len(ONE_AWAY) + 1) * count)], s4.at[1, 0, step])
        via = lax.rem(step, len(ONE_AWAY))
        farthest = last[step, 7 * count :].astype(F32)
        for k, (d, along) in enumerate(zip(ONE_AWAY, ON)):
            here = pl.ds(d * count, count)
            total = part[step, here].astype(F32) + last[step, pl.ds((d + along) * count, count)].astype(F32)
            moved[step, here] = (total + jnp.where(via == k, farthest, 0.0)).astype(BF16)
        for d in ONE_AWAY:
            pass_sums(moved, step, d, d, near[d], 1)
        return carry

    def finish(step, carry):
        wait_for(last.at[step, pl.ds(0, len(ONE_AWAY) * count)], s4.at[1, 1, step])
        total = part[step, :count].astype(F32)
        for d in ONE_AWAY:
            total = total + last[step, d * count : (d + 1) * count].astype(F32)
        out[:, feature_span(step)] = total.astype(BF16)
        return carry

    lax.fori_loop(0, steps, combine, 0)
    lax.fori_loop(0, relayed, relay, 0)

    def finish_direct(step, carry):
        wait_for(last.at[step, pl.ds(count, (CUBE - 1) * count)], s4.at[1, 0, step])
        total = part[step, :count].astype(F32)
        for d in range(1, CUBE):
            total = total + last[step, d * count : (d + 1) * count].astype(F32)
        out[:, feature_span(step)] = total.astype(BF16)
        return carry

    lax.fori_loop(0, relayed, finish, 0)
    lax.fori_loop(relayed, steps, finish_direct, 0)

    for phase in range(2):
        wait_for(table.at[pl.ds(0, len(ONE_AWAY) + phase)], table_sems.at[0, phase])

    def drain(step, carry):
        for phase in range(2):
            moved_rows = pl.ds(0, (len(ONE_AWAY) + 1 - phase) * count)
            wait_for(held.at[step, pl.ds(0, (len(ONE_AWAY) + phase) * count)], s1.at[0, phase, step])

            @pl.when(step < relayed)
            def _():
                wait_for(part.at[step, moved_rows], s4.at[0, phase, step])

        @pl.when(step >= relayed)
        def _():
            wait_for(part.at[step, pl.ds(count, (CUBE - 1) * count)], s4.at[0, 0, step])

        for across in range(2):
            wait_for(sent.at[step, half_span(across)], s2.at[0, across, step])
            wait_for(made.at[step, half_span(across)], s3.at[0, across, step])
        for which in range(3):
            weight_send(which, step).wait_send()
        return carry

    lax.fori_loop(0, steps, drain, 0)


def body(tokens, gate_weights, expert_ids, w_gate, w_up, w_down):
    count, features = tokens.shape
    choices = expert_ids.shape[1]
    units = w_gate.shape[2]
    steps = features // STEP
    gathered = CUBE * count
    slots = 2 * CUBE * CUBE * MOST
    dma = pltpu.SemaphoreType.DMA
    whole = pl.BlockSpec(memory_space=pl.ANY)
    vmem = pl.BlockSpec(memory_space=pltpu.VMEM)
    return pl.pallas_call(
        kernel,
        out_shape=pltpu.VMEM((count, features), BF16),
        in_specs=[whole, whole, whole, whole, whole, whole],
        out_specs=vmem,
        scratch_shapes=[
            pltpu.VMEM((steps, gathered, STEP), BF16),
            pltpu.VMEM((CUBE, 2 * count, 128), BF16),
            pltpu.VMEM((slots, gathered), BF16),
            pltpu.VMEM((gathered, slots), BF16),
            pltpu.VMEM((steps, slots, STEP), BF16),
            pltpu.VMEM((steps, slots, STEP), BF16),
            pltpu.VMEM((slots, 2 * units), F32),
            pltpu.VMEM((slots, 2 * units), F32),
            pltpu.VMEM((slots, 2 * units), BF16),
            pltpu.VMEM((steps, slots, STEP), BF16),
            pltpu.VMEM((steps, slots, STEP), BF16),
            pltpu.VMEM((steps, gathered, STEP), BF16),
            pltpu.VMEM((steps, gathered, STEP), BF16),
            pltpu.VMEM((steps, gathered, STEP), BF16),
            pltpu.VMEM((steps, 2, STEP, units), BF16),
            pltpu.VMEM((steps, 2, STEP, units), BF16),
            pltpu.VMEM((steps, 2, STEP, units), BF16),
            pltpu.VMEM((choices, count), BF16),
            pltpu.VMEM((choices, count), jnp.int32),
            pltpu.SemaphoreType.REGULAR((3,)),
            dma((2,)),
            dma((steps,)),
            dma((2, 2)),
            dma((2, 2, steps)),
            dma((2, 2, steps)),
            dma((2, 2, steps)),
            dma((2, 2, steps)),
            dma((3, steps)),
            dma((3, steps)),
            dma((3, steps)),
        ],
        compiler_params=pltpu.CompilerParams(
            collective_id=0, has_side_effects=True, vmem_limit_bytes=54_000_000
        ),
    )(*(pltpu.with_memory_space_constraint(x, pltpu.HBM) for x in (tokens, gate_weights.T, expert_ids.T, w_gate, w_up, w_down)))


def solution(mesh):
    placed = (
        P(("grp", "loc"), None),
        P(("grp", "loc"), None),
        P(("grp", "loc"), None),
        P("grp", None, "loc"),
        P("grp", None, "loc"),
        P("grp", None, "loc"),
    )
    return jax.shard_map(
        body, mesh=mesh, in_specs=placed, out_specs=P(("grp", "loc"), None), check_vma=False
    )
```
